256 devices in a mesh: ep: 64 (over z, y, core), fsdp: 4 (over x).
Axes of the slice: x: 4, y: 4, z: 8, core: 2. Of those that a mesh axis runs over, the one named last changes fastest.
Arguments:
- train_gate: float32 [64, 2048, 1024], P('ep', 'fsdp'), may hold values from -0.1875 to 0.1875
- other_gate: bfloat16 [64, 2048, 1024], P('ep', 'fsdp'), may hold values from -0.0625 to 0.0625
- train_up: float32 [64, 2048, 1024], P('ep', 'fsdp'), may hold values from -0.1875 to 0.1875
- other_up: bfloat16 [64, 2048, 1024], P('ep', 'fsdp'), may hold values from -0.0625 to 0.0625
- router_weight: float32 [2048, 64], P('fsdp', 'ep'), may hold values from -0.125 to 0.125
- router_gain: float32 [2048], P('fsdp'), may hold values from 0.25 to 1.75
Outputs:
- ready_gate: bfloat16 [64, 2048, 1024], P('ep')
- ready_up: bfloat16 [64, 2048, 1024], P('ep')
- scale_gate: float32 [64, 1024], P('ep')
- scale_up: float32 [64, 1024], P('ep')
- serve_router: bfloat16 [2048, 64], replicated
The draws below stay inside these ranges and needn't reach their ends.
All inputs are finite; a program needn't handle non-finite values.
Results may differ from the reference program's by a relative error of at most 0.001.
Values may be sent and summed in bfloat16 or wider, within the bound.
No kernel may reach another device: no remote copies, remote signals or barrier semaphores. Data moves between devices by JAX's collectives and lax.ppermute only.
A program may use at most 64 MiB of HBM per device.

```python
import jax
import jax.numpy as jnp
from jax import lax

EXPERTS = 64
D_MODEL = 2048
D_EXPERT = 1024


def strengthened(drawn, key, source, target, shards_of, factor):
    owner, partner = [(jnp.arange(drawn.shape[dim]) // (drawn.shape[dim] // shards_of)).reshape([-1 if axis == dim else 1 for axis in range(drawn.ndim)]) for dim in (source, target)]
    chosen = jax.random.permutation(key, shards_of)[partner]
    strong = (owner == chosen) | (owner == (partner + shards_of // 2) % shards_of)
    return jnp.where(strong, factor * drawn, drawn)


def shard_levels(stream_key, dims, pieces, low, top_value):
    level = 1.0
    for dim, shards_of in pieces:
        steps = jax.random.uniform(jax.random.fold_in(jax.random.fold_in(stream_key, 6), dim), (shards_of,), jnp.float32, low / len(pieces), top_value / len(pieces))
        level = level * jnp.repeat(jnp.exp(steps), dims[dim] // shards_of).reshape((-1,) + (1,) * (len(dims) - 1 - dim))
    return level


def normal_values(own_key, extent, width, most, split=(), dtype=jnp.bfloat16):
    factor_of = shard_levels(own_key, extent, split, -0.22, 0.18) if split else 1.0
    result = jax.random.normal(own_key, extent, jnp.float32) * width * factor_of
    return jnp.minimum(jnp.maximum(result, -most), most).astype(dtype)


def gaussian_with(key, extent, deviation, most, cuts, heavy, held_as=jnp.bfloat16):
    array = deviation * jax.random.normal(key, extent, jnp.float32)
    if cuts:
        array = array * shard_levels(key, extent, cuts, -0.22, 0.18)
    return jnp.clip(strengthened(array, jax.random.fold_in(key, 3), *heavy), -most, most).astype(held_as)


def setup_inputs(seed: int = 0) -> dict:
    streams_of = jax.random.split(jax.random.key(seed), 7)
    return {
        "train_gate": gaussian_with(streams_of[0], (EXPERTS, D_MODEL, D_EXPERT), D_MODEL ** -0.5, 0.1875, ((0, 64), (1, 4)), (1, 2, 4, 2.0), jnp.float32),
        "other_gate": normal_values(streams_of[1], (EXPERTS, D_MODEL, D_EXPERT), (D_MODEL * 4) ** -0.5, 0.0625, ((0, 64), (1, 4))),
        "train_up": gaussian_with(streams_of[2], (EXPERTS, D_MODEL, D_EXPERT), D_MODEL ** -0.5, 0.1875, ((0, 64), (1, 4)), (1, 2, 4, 2.0), jnp.float32),
        "other_up": normal_values(streams_of[3], (EXPERTS, D_MODEL, D_EXPERT), (D_MODEL * 4) ** -0.5, 0.0625, ((0, 64), (1, 4))),
        "router_weight": normal_values(streams_of[4], (D_MODEL, EXPERTS), D_MODEL ** -0.5, 0.125, ((0, 4), (1, 64)), jnp.float32),
        "router_gain": jnp.clip(1.0 + 0.15 * jax.random.normal(streams_of[5], (D_MODEL,), jnp.float32), 0.25, 1.75),
    }


def reference(train_gate, other_gate, train_up, other_up, router_weight, router_gain):
    latest_gate = train_gate + other_gate.astype(jnp.float32)
    latest_up = train_up + other_up.astype(jnp.float32)
    scale_gate = jnp.sqrt(lax.optimization_barrier(jnp.sum(latest_gate * latest_gate, axis=1)))
    ready_gate = (latest_gate / jnp.expand_dims(scale_gate, 1)).astype(jnp.bfloat16)
    scale_up = jnp.sqrt(lax.optimization_barrier(jnp.sum(latest_up * latest_up, axis=1)))
    ready_up = (latest_up / jnp.expand_dims(scale_up, 1)).astype(jnp.bfloat16)
    serve_router = (router_weight * router_gain[:, None]).astype(jnp.bfloat16)
    return (ready_gate, ready_up, scale_gate, scale_up, serve_router)
```

```python
import jax
import jax.numpy as jnp
from jax import lax
from jax.sharding import PartitionSpec as P


def body(train_gate, other_gate, train_up, other_up, router_weight, router_gain):
    n = lax.axis_size("fsdp")
    me = lax.axis_index("fsdp")
    rows, cols = train_gate.shape[1:]

    def shifted(value, by):
        return lax.ppermute(value, "fsdp", [(i, (i + by) % n) for i in range(n)])

    latest = [t[0] + o[0].astype(jnp.float32) for t, o in ((train_gate, other_gate), (train_up, other_up))]
    sums = [jnp.sum(v * v, axis=0) for v in latest]
    small = jnp.concatenate([*sums, router_weight[:, 0] * router_gain])
    small = lax.all_to_all(jnp.broadcast_to(small, (n, small.size)), "fsdp", split_axis=0, concat_axis=0, tiled=True)
    scale = jnp.sqrt(jnp.sum(small[:, : 2 * cols], axis=0)).reshape(2, cols)
    gate, up = [(v / scale[k]).astype(jnp.bfloat16) for k, v in enumerate(latest)]

    gate_left = shifted(gate, 1)
    up_right = shifted(up, n - 1)
    up_left = shifted(up, 1)
    gate_right = shifted(gate, n - 1)
    gate_far = shifted(gate_left, 1)
    up_far = shifted(up_right, n - 1)
    row_router = small[:, 2 * cols :].reshape(-1).astype(jnp.bfloat16)
    e = lax.axis_size("ep")
    copies = jnp.broadcast_to(row_router, (e, row_router.size))
    serve_router = lax.all_to_all(copies, "ep", split_axis=0, concat_axis=0, tiled=True).T

    outs = []
    for own, lefts, rights, far in ((gate, gate_left, gate_right, gate_far), (up, up_left, up_right, up_far)):
        buf = jnp.zeros((n * rows, cols), jnp.bfloat16)
        for piece, by in ((own, 0), (lefts, n - 1), (rights, 1), (far, 2)):
            buf = lax.dynamic_update_slice(buf, piece, ((me + by) % n * rows, 0))
        outs.append(buf[None])
    return (outs[0], outs[1], scale[0:1], scale[1:2], serve_router)


def solution(mesh):
    placed = (
        P("ep", "fsdp", None),
        P("ep", "fsdp", None),
        P("ep", "fsdp", None),
        P("ep", "fsdp", None),
        P("fsdp", "ep"),
        P("fsdp"),
    )
    return jax.shard_map(
        body,
        mesh=mesh,
        in_specs=placed,
        out_specs=(P("ep", None, None), P("ep", None, None), P("ep", None), P("ep", None), P()),
        check_vma=False,
    )
```

```python
import functools

import jax
import jax.numpy as jnp
from jax import lax
from jax.experimental import pallas as pl
from jax.experimental.pallas import tpu as pltpu
from jax.sharding import PartitionSpec as P


RAW = 48
GATE_LAST, UP_LAST, UP_RIGHT = 96, 96, 16
STEP = 64
VMEM = pl.BlockSpec(memory_space=pltpu.VMEM)
ANY = pl.BlockSpec(memory_space=pl.ANY)


def in_vmem(x):
    return pltpu.with_memory_space_constraint(x, pltpu.VMEM)


def in_hbm(x):
    return pltpu.with_memory_space_constraint(x, pltpu.HBM)


def sums_kernel(train_gate, other_gate, train_up, other_up, weight, gain, small, raw, gate, up, train, other, router, sems):
    rows, cols = gate.shape
    steps = rows // STEP
    sources = ((train_gate, other_gate), (train_up, other_up))

    def copies(k, i):
        at = pl.ds(i * STEP, STEP)
        return [
            pltpu.make_async_copy(hbm.at[at], held.at[k, at], sems.at[k, i])
            for hbm, held in zip(sources[k], (train, other))
        ]

    rest = [pltpu.make_async_copy(v, router.at[k], sems.at[2, k]) for k, v in enumerate((weight, gain))]
    for k in range(2):
        for i in range(steps):
            for c in copies(k, i):
                c.start()
        if k == 0:
            for c in rest:
                c.start()
    small[2:] = jnp.zeros((small.shape[0] - 2, cols), jnp.float32)
    for k, latest in enumerate((gate, up)):
        total = jnp.zeros((8, cols), jnp.float32)
        for i in range(steps):
            for c in copies(k, i):
                c.wait()

            def add(j, total):
                at = pl.ds(pl.multiple_of(i * STEP + j * 16, 16), 16)
                v = train[k, at, :] + other[k, at, :].astype(jnp.float32)
                latest[at, :] = v
                return total + (v[:8] * v[:8] + v[8:] * v[8:])

            total = lax.fori_loop(0, STEP // 16, add, total, unroll=True)
            if k == 0 and i == pl.cdiv(RAW, STEP) - 1:
                raw[...] = gate[:RAW]
        small[k : k + 1, :] = jnp.sum(total, axis=0, keepdims=True)
    for c in rest:
        c.wait()
    small[2:3, : weight.shape[1]] = router[0] * router[1]


def sums(*args):
    rows, cols = args[0].shape
    f32 = jnp.float32
    return pl.pallas_call(
        sums_kernel,
        out_shape=(
            pltpu.VMEM((4, cols), f32),
            pltpu.VMEM((RAW, cols), f32),
            pltpu.VMEM((rows, cols), f32),
            pltpu.VMEM((rows, cols), f32),
        ),
        in_specs=[ANY] * 6,
        out_specs=(VMEM,) * 4,
        scratch_shapes=[
            pltpu.VMEM((2, rows, cols), f32),
            pltpu.VMEM((2, rows, cols), jnp.bfloat16),
            pltpu.VMEM((2, *args[4].shape), f32),
            pltpu.SemaphoreType.DMA((3, rows // STEP)),
        ],
        compiler_params=pltpu.CompilerParams(vmem_limit_bytes=20 << 20),
        name="sums",
        cost_estimate=pl.CostEstimate(flops=8 * rows * cols, bytes_accessed=12 * rows * cols, transcendentals=0),
    )(*map(in_hbm, args))


def ready_kernel(row, own, across, left, right, latest, *outs):
    pieces, scale = outs[:-1], outs[-1]
    at = slice(row, row + 1)
    scale[...] = jnp.sqrt((own[at] + across[at]) + (left[at] + right[at]))
    by = scale[...]
    start = 0
    for ref in pieces:

        def divide(j, _, ref=ref, start=start):
            to = pl.ds(pl.multiple_of(j * 16, 16), 16)
            at = pl.ds(pl.multiple_of(start + j * 16, 16), 16)
            ref[to, :] = (latest[at, :] / by).astype(jnp.bfloat16)
            return 0

        lax.fori_loop(0, ref.shape[0] // 16, divide, 0, unroll=2)
        start += ref.shape[0]


def make_ready(row, parts, latest, sizes, near=None):
    rows, cols = latest.shape
    *pieces, scale = pl.pallas_call(
        functools.partial(ready_kernel, row),
        out_shape=(
            *((pltpu.VMEM if size == near else pltpu.HBM)((size, cols), jnp.bfloat16) for size in sizes),
            pltpu.VMEM((1, cols), jnp.float32),
        ),
        in_specs=[VMEM] * 5,
        out_specs=(VMEM,) * (len(sizes) + 1),
        compiler_params=pltpu.CompilerParams(vmem_limit_bytes=8 << 20),
        name="ready",
        cost_estimate=pl.CostEstimate(flops=2 * rows * cols, bytes_accessed=2 * cols, transcendentals=0),
    )(*map(in_vmem, parts), in_vmem(latest))
    return pieces, scale


def place_kernel(rows, count, spots, *refs):
    scratch = 1 + sum(staged for *_, staged in spots)
    outs = refs[-count - scratch : -scratch]
    held, sems = list(refs[-scratch:-1]), refs[-1]
    n = outs[0].shape[0] // rows
    me = lax.axis_index("fsdp")
    ins, copies = [], []
    for k, (out, by, at, staged) in enumerate(spots):
        piece = refs[k]
        if staged:
            stage = held.pop(0)
            ins.append(pltpu.make_async_copy(piece, stage, sems.at[1, k]))
            piece = stage
        else:
            ins.append(None)
        block = lax.rem(me + by, n)
        to = pl.ds(pl.multiple_of(block * rows + at, 16), piece.shape[0])
        copies.append(pltpu.make_async_copy(piece, outs[out].at[to], sems.at[0, k]))
    for c in ins:
        if c is not None:
            c.start()
    for i, c in zip(ins, copies):
        if i is not None:
            i.wait()
        c.start()
    for c in copies:
        c.wait()


def place(rows, n, outs, pieces, staged):
    values = [p[0] for p in pieces]
    used = sorted({p[1] for p in pieces})
    spots = tuple((used.index(p[1]), p[2], p[3], staged) for p in pieces)
    cols = values[0].shape[1]
    given = [outs[k] for k in used if outs[k] is not None]
    done = pl.pallas_call(
        functools.partial(place_kernel, rows, len(used), spots),
        out_shape=tuple(pltpu.HBM((n * rows, cols), jnp.bfloat16) for _ in used),
        in_specs=[ANY if staged else VMEM] * len(values) + [ANY] * len(given),
        out_specs=(ANY,) * len(used),
        scratch_shapes=[
            *(pltpu.VMEM(v.shape, v.dtype) for v in values if staged),
            pltpu.SemaphoreType.DMA((2, len(values))),
        ],
        input_output_aliases={len(values) + k: k for k in range(len(given))},
        compiler_params=pltpu.CompilerParams(vmem_limit_bytes=8 << 20),
        name="place",
        cost_estimate=pl.CostEstimate(
            flops=0, bytes_accessed=sum(2 * v.size * 2 for v in values), transcendentals=0
        ),
    )(*map(in_hbm if staged else in_vmem, values), *map(in_hbm, given))
    outs = list(outs)
    for k, v in zip(used, done):
        outs[k] = v
    return outs


def body(train_gate, other_gate, train_up, other_up, router_weight, router_gain):
    n = lax.axis_size("fsdp")
    rows, _ = train_gate.shape[1:]

    def shifted(value, by):
        return lax.ppermute(value, "fsdp", [(i, (i + by) % n) for i in range(n)])

    small, raw, gate, up = sums(
        train_gate[0],
        other_gate[0],
        train_up[0],
        other_up[0],
        router_weight.reshape(1, -1),
        router_gain.reshape(1, -1),
    )
    parts = (small, shifted(small, 2), shifted(small, 1), shifted(small, n - 1))
    raw_left = shifted(raw, 1)
    raw_right = shifted(raw, n - 1)
    gate_sizes = (RAW, rows - RAW - GATE_LAST, GATE_LAST)
    up_sizes = (rows - UP_LAST - UP_RIGHT, UP_LAST, UP_RIGHT)
    (head, gate0, gate1), scale_gate = make_ready(0, parts, gate, gate_sizes, gate_sizes[1])
    left_gate0 = shifted(gate0, 1)
    right_gate0 = shifted(gate0, n - 1)
    (up0, up1, up2), scale_up = make_ready(1, parts, up, up_sizes)
    left_up, right_up = [], []
    for k, v in enumerate((up0, up1, up2), 1):
        left_up.append(shifted(v, 1))
        right_up.append(shifted(v, n - 1))
    left_gate1 = shifted(gate1, 1)
    right_gate1 = shifted(gate1, n - 1)

    far_gate0 = shifted(left_gate0, 1)
    far_up0 = shifted(right_up[0], n - 1)
    far_up2 = shifted(left_up[2], 1)
    far_up1 = shifted(right_up[1], n - 1)
    far_gate1 = shifted(left_gate1, 1)

    own, across, left, right = [v[2, :rows].astype(jnp.bfloat16) for v in parts]
    turned = jnp.concatenate([own, right, across, left] * 2)
    turned, raw_left, raw_right = lax.optimization_barrier((turned, raw_left, raw_right))
    left_head, right_head = [(v / scale_gate).astype(jnp.bfloat16) for v in (raw_left, raw_right)]
    far_head = shifted(left_head, 1)
    row_router = lax.dynamic_slice(turned, ((n - lax.axis_index("fsdp")) % n * rows,), (n * rows,))
    e = lax.axis_size("ep")
    copies = jnp.broadcast_to(row_router, (e, row_router.size))
    serve_router = lax.all_to_all(copies, "ep", split_axis=0, concat_axis=0, tiled=True).T

    at_gate = (0, RAW, rows - GATE_LAST)
    at_up = (0, rows - UP_LAST - UP_RIGHT, rows - UP_RIGHT)

    def gates(by, *values):
        return [(v, 0, by, at) for v, at in zip(values, at_gate) if v is not None]

    def ups(by, *values):
        return [(v, 1, by, at) for v, at in zip(values, at_up) if v is not None]

    groups = (
        gates(0, head, gate0, gate1) + ups(0, up0, up1, up2),
        gates(n - 1, left_head, left_gate0) + gates(1, right_head, right_gate0),
        ups(n - 1, *left_up) + ups(1, *right_up) + gates(n - 1, None, None, left_gate1) + gates(1, None, None, right_gate1),
        gates(2, far_head, far_gate0) + ups(2, far_up0, None, far_up2),
        gates(2, None, None, far_gate1) + ups(2, None, far_up1),
    )
    outs = [None, None]
    for k, group in enumerate(groups):
        outs = place(rows, n, outs, group, k < 3)
    return (outs[0][None], outs[1][None], scale_gate, scale_up, serve_router)


def solution(mesh):
    placed = (
        P("ep", "fsdp", None),
        P("ep", "fsdp", None),
        P("ep", "fsdp", None),
        P("ep", "fsdp", None),
        P("fsdp", "ep"),
        P("fsdp"),
    )
    return jax.shard_map(
        body,
        mesh=mesh,
        in_specs=placed,
        out_specs=(P("ep", None, None), P("ep", None, None), P("ep", None), P("ep", None), P()),
        check_vma=False,
    )
```

```python
import functools

import jax
import jax.numpy as jnp
from jax import lax
from jax.experimental import pallas as pl
from jax.experimental.pallas import tpu as pltpu
from jax.sharding import PartitionSpec as P


RAW_NEAR, RAW_WIDE = 64, 48
GATE_LAST, UP_LAST = 96, 96
STEP = 64
LANES = 128
VMEM = pl.BlockSpec(memory_space=pltpu.VMEM)
ANY = pl.BlockSpec(memory_space=pl.ANY)


def in_vmem(x):
    return pltpu.with_memory_space_constraint(x, pltpu.VMEM)


def in_hbm(x):
    return pltpu.with_memory_space_constraint(x, pltpu.HBM)


def sums_kernel(train_gate, other_gate, train_up, other_up, weight, gain, small, raw_near, raw_wide, gate, up, train, other, router, sems):
    rows, cols = up.shape
    steps = rows // STEP
    sources = ((train_gate, other_gate), (train_up, other_up))

    def copies(k, i):
        at = pl.ds(i * STEP, STEP)
        return [
            pltpu.make_async_copy(hbm.at[at], held.at[k, at], sems.at[k, i])
            for hbm, held in zip(sources[k], (train, other))
        ]

    rest = [pltpu.make_async_copy(v, router.at[k], sems.at[2, k]) for k, v in enumerate((weight, gain))]
    for k in range(2):
        for i in range(steps):
            for c in copies(k, i):
                c.start()
        if k == 0:
            for c in rest:
                c.start()
    small[2:] = jnp.zeros((small.shape[0] - 2, cols), jnp.float32)
    for k in range(2):
        total = jnp.zeros((8, cols), jnp.float32)
        for i in range(steps):
            for c in copies(k, i):
                c.wait()

            for row in range(i * STEP, (i + 1) * STEP, 16):
                v = train[k, row : row + 16, :] + other[k, row : row + 16, :].astype(jnp.float32)
                total += v[:8] * v[:8] + v[8:] * v[8:]
                for ref, first in ((up, 0),) if k else ((raw_near, 0), (raw_wide, 0), (gate, RAW_NEAR)):
                    if first <= row < first + ref.shape[0]:
                        ref[row - first : row - first + 16, :] = v
        small[k : k + 1, :] = jnp.sum(total, axis=0, keepdims=True)
    for c in rest:
        c.wait()
    small[2:3, : weight.shape[1]] = router[0] * router[1]


def sums(*args):
    rows, cols = args[0].shape
    f32 = jnp.float32
    return pl.pallas_call(
        sums_kernel,
        out_shape=(
            pltpu.VMEM((4, cols), f32),
            pltpu.VMEM((RAW_NEAR, cols), f32),
            pltpu.VMEM((RAW_WIDE, cols), f32),
            pltpu.VMEM((rows - RAW_NEAR - GATE_LAST, cols), f32),
            pltpu.VMEM((rows, cols), f32),
        ),
        in_specs=[ANY] * 6,
        out_specs=(VMEM,) * 5,
        scratch_shapes=[
            pltpu.VMEM((2, rows, cols), f32),
            pltpu.VMEM((2, rows, cols), jnp.bfloat16),
            pltpu.VMEM((2, *args[4].shape), f32),
            pltpu.SemaphoreType.DMA((3, rows // STEP)),
        ],
        compiler_params=pltpu.CompilerParams(vmem_limit_bytes=20 << 20),
        name="sums",
        cost_estimate=pl.CostEstimate(flops=8 * rows * cols, bytes_accessed=12 * rows * cols, transcendentals=0),
    )(*map(in_hbm, args))


def pair_kernel(own, near, pair):
    half = own.shape[1] // 2
    pair[:2] = own[:2] + near[:2]
    pair[2:3, :half] = own[2:3, :half]
    pair[2:3, half:] = near[2:3, :half]
    pair[3:4] = jnp.zeros((1, 2 * half), jnp.float32)


def add_pair(own, near):
    return pl.pallas_call(
        pair_kernel,
        out_shape=pltpu.VMEM(own.shape, own.dtype),
        in_specs=[VMEM] * 2,
        out_specs=VMEM,
        compiler_params=pltpu.CompilerParams(vmem_limit_bytes=2 << 20),
        name="pair",
        cost_estimate=pl.CostEstimate(flops=2 * own.size, bytes_accessed=own.size, transcendentals=0),
    )(in_vmem(own), in_vmem(near))


def divided(ref, value, scale):
    def divide(j, _):
        at = pl.ds(pl.multiple_of(j * 16, 16), 16)
        ref[at, :] = (value(at) / scale).astype(jnp.bfloat16)
        return 0

    lax.fori_loop(0, ref.shape[0] // 16, divide, 0, unroll=2)


def first_kernel(pair, wide, gate, gate0, scale):
    scale[...] = jnp.sqrt(pair[:1] + wide[:1])
    divided(gate0, lambda at: gate[at, :], scale[...])


def ready_first(pair, wide, gate):
    return pl.pallas_call(
        first_kernel,
        out_shape=(pltpu.VMEM(gate.shape, jnp.bfloat16), pltpu.VMEM((1, gate.shape[1]), jnp.float32)),
        in_specs=[VMEM] * 3,
        out_specs=(VMEM,) * 2,
        compiler_params=pltpu.CompilerParams(vmem_limit_bytes=4 << 20),
        name="ready_first",
        cost_estimate=pl.CostEstimate(flops=2 * gate.size, bytes_accessed=4096, transcendentals=0),
    )(*map(in_vmem, (pair, wide, gate)))


def rest_kernel(pair, wide, up, train_gate, other_gate, up0, up1, gate1, gate_a, gate_b, scale, train, other, sems):
    pieces = ((gate1, train_gate.shape[0] - gate1.shape[0]), (gate_a, 0), (gate_b, gate_a.shape[0]))
    copies, at = [], 0
    for piece, first in pieces:
        for hbm, held in ((train_gate, train), (other_gate, other)):
            size = piece.shape[0]
            copies.append(
                pltpu.make_async_copy(
                    hbm.at[pl.ds(first, size)], held.at[pl.ds(at, size)], sems.at[len(copies)]
                )
            )
        at += piece.shape[0]
    for c in copies:
        c.start()
    scale_gate = jnp.sqrt(pair[:1] + wide[:1])
    scale[...] = jnp.sqrt(pair[1:2] + wide[1:2])
    start = 0
    for piece in (up0, up1):
        divided(piece, lambda at, start=start: up[pl.ds(pl.multiple_of(start + at.start, 16), 16), :], scale[...])
        start += piece.shape[0]
    for c in copies:
        c.wait()
    start = 0
    for piece, _ in pieces:

        def latest(at, start=start):
            at = pl.ds(pl.multiple_of(start + at.start, 16), 16)
            return train[at, :] + other[at, :].astype(jnp.float32)

        divided(piece, latest, scale_gate)
        start += piece.shape[0]


def ready_rest(pair, wide, up, train_gate, other_gate):
    rows, cols = up.shape
    sizes = (rows - UP_LAST, UP_LAST, GATE_LAST, RAW_WIDE, RAW_NEAR - RAW_WIDE)
    return pl.pallas_call(
        rest_kernel,
        out_shape=(
            *(pltpu.HBM((size, cols), jnp.bfloat16) for size in sizes),
            pltpu.VMEM((1, cols), jnp.float32),
        ),
        in_specs=[VMEM] * 3 + [ANY] * 2,
        out_specs=(VMEM,) * (len(sizes) + 1),
        scratch_shapes=[
            pltpu.VMEM((GATE_LAST + RAW_NEAR, cols), jnp.float32),
            pltpu.VMEM((GATE_LAST + RAW_NEAR, cols), jnp.bfloat16),
            pltpu.SemaphoreType.DMA((6,)),
        ],
        compiler_params=pltpu.CompilerParams(vmem_limit_bytes=8 << 20),
        name="ready_rest",
        cost_estimate=pl.CostEstimate(flops=3 * rows * cols, bytes_accessed=3 * rows * cols, transcendentals=0),
    )(*map(in_vmem, (pair, wide, up)), in_hbm(train_gate), in_hbm(other_gate))


def router_kernel(pair, wide, copies, held):
    me = lax.axis_index("fsdp")
    odd, high = lax.rem(me, 2) == 1, me >= 2
    half = pair.shape[1] // 2
    own, near = pair[2:3, :half], pair[2:3, half:]
    across, far = wide[2:3, :half], wide[2:3, half:]
    first = jnp.where(odd, near, own), jnp.where(odd, own, near)
    second = jnp.where(odd, across, far), jnp.where(odd, far, across)
    order = [jnp.where(high, b, a) for a, b in zip(first + second, second + first)]
    for k, part in enumerate(order):
        for c in range(half // LANES):
            row = k * (half // LANES) + c
            held[row : row + 1, :] = part[:, c * LANES : (c + 1) * LANES]
    value = held[...].astype(jnp.bfloat16)

    def copy(k, _):
        copies[k] = value
        return 0

    lax.fori_loop(0, copies.shape[0], copy, 0, unroll=4)


def router_copies(pair, wide, count):
    rows = 2 * pair.shape[1] // LANES
    return pl.pallas_call(
        router_kernel,
        out_shape=jax.ShapeDtypeStruct((count, rows, LANES), jnp.bfloat16),
        in_specs=[VMEM] * 2,
        out_specs=VMEM,
        scratch_shapes=[pltpu.VMEM((rows, LANES), jnp.float32)],
        compiler_params=pltpu.CompilerParams(vmem_limit_bytes=4 << 20),
        name="router",
        cost_estimate=pl.CostEstimate(flops=count, bytes_accessed=2 * count * rows * LANES, transcendentals=0),
    )(pair, wide)


def place_kernel(rows, count, spots, *refs):
    scratch = 1 + sum(staged for *_, staged in spots)
    outs = refs[-count - scratch : -scratch]
    held, sems = list(refs[-scratch:-1]), refs[-1]
    me = lax.axis_index("fsdp")
    blocks = {"own": me, "near": me + 1 - 2 * lax.rem(me, 2), "wide": 3 - me, "far": lax.rem(me + 2, 4)}
    ins, copies = [], []
    for k, (out, owner, at, staged) in enumerate(spots):
        piece = refs[k]
        if staged:
            stage = held.pop(0)
            ins.append(pltpu.make_async_copy(piece, stage, sems.at[1, k]))
            piece = stage
        else:
            ins.append(None)
        to = pl.ds(pl.multiple_of(blocks[owner] * rows + at, 16), piece.shape[0])
        copies.append(pltpu.make_async_copy(piece, outs[out].at[to], sems.at[0, k]))
    for c in ins:
        if c is not None:
            c.start()
    for i, c in zip(ins, copies):
        if i is not None:
            i.wait()
        c.start()
    for c in copies:
        c.wait()


def place(rows, n, outs, pieces, staged):
    values = [p[0] for p in pieces]
    used = sorted({p[1] for p in pieces})
    spots = tuple((used.index(p[1]), p[2], p[3], staged) for p in pieces)
    cols = values[0].shape[1]
    given = [outs[k] for k in used if outs[k] is not None]
    done = pl.pallas_call(
        functools.partial(place_kernel, rows, len(used), spots),
        out_shape=tuple(pltpu.HBM((n * rows, cols), jnp.bfloat16) for _ in used),
        in_specs=[ANY if staged else VMEM] * len(values) + [ANY] * len(given),
        out_specs=(ANY,) * len(used),
        scratch_shapes=[
            *(pltpu.VMEM(v.shape, v.dtype) for v in values if staged),
            pltpu.SemaphoreType.DMA((2, len(values))),
        ],
        input_output_aliases={len(values) + k: k for k in range(len(given))},
        compiler_params=pltpu.CompilerParams(vmem_limit_bytes=8 << 20),
        name="place",
        cost_estimate=pl.CostEstimate(
            flops=0, bytes_accessed=sum(2 * v.size * 2 for v in values), transcendentals=0
        ),
    )(*map(in_hbm if staged else in_vmem, values), *map(in_hbm, given))
    outs = list(outs)
    for k, v in zip(used, done):
        outs[k] = v
    return outs


def body(train_gate, other_gate, train_up, other_up, router_weight, router_gain):
    n = lax.axis_size("fsdp")
    rows, _ = train_gate.shape[1:]

    def exchanged(name, value):
        flip = 3 if "w" in name else 1
        return lax.ppermute(value, "fsdp", [(i, i ^ flip) for i in range(n)])

    small, raw_near, raw_wide, gate, up = sums(
        train_gate[0],
        other_gate[0],
        train_up[0],
        other_up[0],
        router_weight.reshape(1, -1),
        router_gain.reshape(1, -1),
    )
    small_n = exchanged("sum_n", small)
    raw_n = exchanged("early_n", raw_near)
    pair = add_pair(small, small_n)
    pair_w = exchanged("sum_w", pair)
    raw_w = exchanged("early_w", raw_wide)

    at_gate = (0, RAW_WIDE, RAW_NEAR, rows - GATE_LAST)
    at_up = (0, rows - UP_LAST)
    gate0, scale_gate = ready_first(pair, pair_w, gate)
    gate0_n = exchanged("n0", gate0)
    gate0_w = exchanged("w0", gate0)
    up0, up1, gate1, gate_a, gate_b, scale_up = ready_rest(pair, pair_w, up, train_gate[0], other_gate[0])
    up0_n, up1_n, gate1_n = [exchanged(f"n{k}", v) for k, v in enumerate((up0, up1, gate1), 1)]
    gate_b_w, up0_w, up1_w, gate1_w = [exchanged(f"w{k}", v) for k, v in enumerate((gate_b, up0, up1, gate1), 1)]

    late, late_w, raw_n, raw_w, _ = lax.optimization_barrier((pair, pair_w, raw_n, raw_w, up1))
    copies = router_copies(late, late_w, lax.axis_size("ep"))
    columns = lax.all_to_all(copies, "ep", split_axis=0, concat_axis=0, tiled=True)
    serve_router = columns.reshape(columns.shape[0], -1).T

    gate_a_n, gate_b_n, gate_a_w = [
        (v / scale_gate).astype(jnp.bfloat16) for v in (raw_n[:RAW_WIDE], raw_n[RAW_WIDE:], raw_w)
    ]
    far_gate0 = exchanged("far_w0", gate0_n)
    far_up0 = exchanged("far_n0", up0_w)
    far_gate_b = exchanged("far_w1", gate_b_n)
    far_gate_a = exchanged("far_n1", gate_a_w)
    far_up1 = exchanged("far_n2", up1_w)
    far_gate1 = exchanged("far_w2", gate1_n)

    def gates(owner, *values):
        return [(v, 0, owner, at) for v, at in zip(values, at_gate) if v is not None]

    def ups(owner, *values):
        return [(v, 1, owner, at) for v, at in zip(values, at_up) if v is not None]

    groups = (
        gates("own", gate_a, gate_b, gate0, gate1) + ups("own", up0, up1),
        gates("near", gate_a_n, gate_b_n, gate0_n) + gates("wide", gate_a_w, gate_b_w, gate0_w),
        gates("near", None, None, None, gate1_n)
        + gates("wide", None, None, None, gate1_w)
        + ups("near", up0_n, up1_n)
        + ups("wide", up0_w, up1_w),
        gates("far", far_gate_a, far_gate_b, far_gate0) + ups("far", far_up0),
        gates("far", None, None, None, far_gate1) + ups("far", None, far_up1),
    )
    outs = [None, None]
    for k, group in enumerate(groups):
        outs = place(rows, n, outs, group, k < 3)
    return (outs[0][None], outs[1][None], scale_gate, scale_up, serve_router)


def solution(mesh):
    placed = (
        P("ep", "fsdp", None),
        P("ep", "fsdp", None),
        P("ep", "fsdp", None),
        P("ep", "fsdp", None),
        P("fsdp", "ep"),
        P("fsdp"),
    )
    return jax.shard_map(
        body,
        mesh=mesh,
        in_specs=placed,
        out_specs=(P("ep", None, None), P("ep", None, None), P("ep", None), P("ep", None), P()),
        check_vma=False,
    )
```

```python
import functools

import jax
import jax.numpy as jnp
from jax import lax
from jax.experimental import pallas as pl
from jax.experimental.pallas import tpu as pltpu
from jax.sharding import PartitionSpec as P


RAW_NEAR, RAW_WIDE = 64, 48
GATE_LAST, UP_LAST = 96, 96
STEPS = (512,), (256, 192, 64)
LANES = 128
VMEM = pl.BlockSpec(memory_space=pltpu.VMEM)
ANY = pl.BlockSpec(memory_space=pl.ANY)


def in_vmem(x):
    return pltpu.with_memory_space_constraint(x, pltpu.VMEM)


def in_hbm(x):
    return pltpu.with_memory_space_constraint(x, pltpu.HBM)


def sums_kernel(train_gate, other_gate, train_up, other_up, weight, gain, small, raw_near, raw_wide, gate, up, train, other, router, sems):
    cols = up.shape[1]
    sources = ((train_gate, other_gate), (train_up, other_up))

    def copies(k, i):
        at = pl.ds(sum(STEPS[k][:i]), STEPS[k][i])
        return [
            pltpu.make_async_copy(hbm.at[at], held.at[k, at], sems.at[k, i])
            for hbm, held in zip(sources[k], (train, other))
        ]

    rest = [pltpu.make_async_copy(v, router.at[k], sems.at[2, k]) for k, v in enumerate((weight, gain))]
    for k in range(2):
        for i in range(len(STEPS[k])):
            for c in copies(k, i):
                c.start()
        if k == 0:
            for c in rest:
                c.start()
    small[2:] = jnp.zeros((small.shape[0] - 2, cols), jnp.float32)
    for k in range(2):
        total = jnp.zeros((8, cols), jnp.float32)
        for i, size in enumerate(STEPS[k]):
            for c in copies(k, i):
                c.wait()
            start = sum(STEPS[k][:i])
            for row in range(start, start + size, 16):
                v = train[k, row : row + 16, :] + other[k, row : row + 16, :].astype(jnp.float32)
                total += v[:8] * v[:8] + v[8:] * v[8:]
                for ref, first in ((up, 0),) if k else ((raw_near, 0), (raw_wide, 0), (gate, RAW_NEAR)):
                    if first <= row < first + ref.shape[0]:
                        ref[row - first : row - first + 16, :] = v
        small[k : k + 1, :] = jnp.sum(total, axis=0, keepdims=True)
    for c in rest:
        c.wait()
    small[2:3, : weight.shape[1]] = router[0] * router[1]


def sums(*args):
    rows, cols = args[0].shape
    f32 = jnp.float32
    return pl.pallas_call(
        sums_kernel,
        out_shape=(
            pltpu.VMEM((4, cols), f32),
            pltpu.VMEM((RAW_NEAR, cols), f32),
            pltpu.VMEM((RAW_WIDE, cols), f32),
            pltpu.VMEM((rows - RAW_NEAR - GATE_LAST, cols), f32),
            pltpu.VMEM((rows, cols), f32),
        ),
        in_specs=[ANY] * 6,
        out_specs=(VMEM,) * 5,
        scratch_shapes=[
            pltpu.VMEM((2, rows, cols), f32),
            pltpu.VMEM((2, rows, cols), jnp.bfloat16),
            pltpu.VMEM((2, *args[4].shape), f32),
            pltpu.SemaphoreType.DMA((3, max(map(len, STEPS)))),
        ],
        compiler_params=pltpu.CompilerParams(vmem_limit_bytes=20 << 20),
        name="sums",
        cost_estimate=pl.CostEstimate(flops=8 * rows * cols, bytes_accessed=12 * rows * cols, transcendentals=0),
    )(*map(in_hbm, args))


def pair_kernel(own, near, pair):
    half = own.shape[1] // 2
    pair[:2] = own[:2] + near[:2]
    pair[2:3, :half] = own[2:3, :half]
    pair[2:3, half:] = near[2:3, :half]
    pair[3:4] = jnp.zeros((1, 2 * half), jnp.float32)


def add_pair(own, near):
    return pl.pallas_call(
        pair_kernel,
        out_shape=pltpu.VMEM(own.shape, own.dtype),
        in_specs=[VMEM] * 2,
        out_specs=VMEM,
        compiler_params=pltpu.CompilerParams(vmem_limit_bytes=2 << 20),
        name="pair",
        cost_estimate=pl.CostEstimate(flops=2 * own.size, bytes_accessed=own.size, transcendentals=0),
    )(in_vmem(own), in_vmem(near))


def divided(ref, value, scale):
    def divide(j, _):
        at = pl.ds(pl.multiple_of(j * 16, 16), 16)
        ref[at, :] = (value(at) / scale).astype(jnp.bfloat16)
        return 0

    lax.fori_loop(0, ref.shape[0] // 16, divide, 0, unroll=2)


def first_kernel(pair, wide, gate, gate0, scale):
    scale[...] = jnp.sqrt(pair[:1] + wide[:1])
    divided(gate0, lambda at: gate[at, :], scale[...])


def ready_first(pair, wide, gate):
    return pl.pallas_call(
        first_kernel,
        out_shape=(pltpu.VMEM(gate.shape, jnp.bfloat16), pltpu.VMEM((1, gate.shape[1]), jnp.float32)),
        in_specs=[VMEM] * 3,
        out_specs=(VMEM,) * 2,
        compiler_params=pltpu.CompilerParams(vmem_limit_bytes=4 << 20),
        name="ready_first",
        cost_estimate=pl.CostEstimate(flops=2 * gate.size, bytes_accessed=4096, transcendentals=0),
    )(*map(in_vmem, (pair, wide, gate)))


def rest_kernel(pair, wide, up, train_gate, other_gate, up0, up1, gate1, gate_a, gate_b, scale, train, other, sems):
    pieces = ((gate1, train_gate.shape[0] - gate1.shape[0]), (gate_a, 0), (gate_b, gate_a.shape[0]))
    copies, at = [], 0
    for piece, first in pieces:
        for hbm, held in ((train_gate, train), (other_gate, other)):
            size = piece.shape[0]
            copies.append(
                pltpu.make_async_copy(
                    hbm.at[pl.ds(first, size)], held.at[pl.ds(at, size)], sems.at[len(copies)]
                )
            )
        at += piece.shape[0]
    for c in copies:
        c.start()
    scale_gate = jnp.sqrt(pair[:1] + wide[:1])
    scale[...] = jnp.sqrt(pair[1:2] + wide[1:2])
    start = 0
    for piece in (up0, up1):
        divided(piece, lambda at, start=start: up[pl.ds(pl.multiple_of(start + at.start, 16), 16), :], scale[...])
        start += piece.shape[0]
    for c in copies:
        c.wait()
    start = 0
    for piece, _ in pieces:

        def latest(at, start=start):
            at = pl.ds(pl.multiple_of(start + at.start, 16), 16)
            return train[at, :] + other[at, :].astype(jnp.float32)

        divided(piece, latest, scale_gate)
        start += piece.shape[0]


def ready_rest(pair, wide, up, train_gate, other_gate):
    rows, cols = up.shape
    sizes = (rows - UP_LAST, UP_LAST, GATE_LAST, RAW_WIDE, RAW_NEAR - RAW_WIDE)
    return pl.pallas_call(
        rest_kernel,
        out_shape=(
            *(pltpu.HBM((size, cols), jnp.bfloat16) for size in sizes),
            pltpu.VMEM((1, cols), jnp.float32),
        ),
        in_specs=[VMEM] * 3 + [ANY] * 2,
        out_specs=(VMEM,) * (len(sizes) + 1),
        scratch_shapes=[
            pltpu.VMEM((GATE_LAST + RAW_NEAR, cols), jnp.float32),
            pltpu.VMEM((GATE_LAST + RAW_NEAR, cols), jnp.bfloat16),
            pltpu.SemaphoreType.DMA((6,)),
        ],
        compiler_params=pltpu.CompilerParams(vmem_limit_bytes=8 << 20),
        name="ready_rest",
        cost_estimate=pl.CostEstimate(flops=3 * rows * cols, bytes_accessed=3 * rows * cols, transcendentals=0),
    )(*map(in_vmem, (pair, wide, up)), in_hbm(train_gate), in_hbm(other_gate))


def router_kernel(pair, wide, copies, held):
    me = lax.axis_index("fsdp")
    odd, high = lax.rem(me, 2) == 1, me >= 2
    half = pair.shape[1] // 2
    own, near = pair[2:3, :half], pair[2:3, half:]
    across, far = wide[2:3, :half], wide[2:3, half:]
    first = jnp.where(odd, near, own), jnp.where(odd, own, near)
    second = jnp.where(odd, across, far), jnp.where(odd, far, across)
    order = [jnp.where(high, b, a) for a, b in zip(first + second, second + first)]
    for k, part in enumerate(order):
        for c in range(half // LANES):
            row = k * (half // LANES) + c
            held[row : row + 1, :] = part[:, c * LANES : (c + 1) * LANES]
    value = held[...].astype(jnp.bfloat16)

    def copy(k, _):
        copies[k] = value
        return 0

    lax.fori_loop(0, copies.shape[0], copy, 0, unroll=4)


def router_copies(pair, wide, count):
    rows = 2 * pair.shape[1] // LANES
    return pl.pallas_call(
        router_kernel,
        out_shape=jax.ShapeDtypeStruct((count, rows, LANES), jnp.bfloat16),
        in_specs=[VMEM] * 2,
        out_specs=VMEM,
        scratch_shapes=[pltpu.VMEM((rows, LANES), jnp.float32)],
        compiler_params=pltpu.CompilerParams(vmem_limit_bytes=4 << 20),
        name="router",
        cost_estimate=pl.CostEstimate(flops=count, bytes_accessed=2 * count * rows * LANES, transcendentals=0),
    )(pair, wide)


def place_kernel(rows, count, spots, *refs):
    scratch = 1 + sum(staged for *_, staged in spots)
    outs = refs[-count - scratch : -scratch]
    held, sems = list(refs[-scratch:-1]), refs[-1]
    me = lax.axis_index("fsdp")
    blocks = {"own": me, "near": me + 1 - 2 * lax.rem(me, 2), "wide": 3 - me, "far": lax.rem(me + 2, 4)}
    ins, copies = [], []
    for k, (out, owner, at, staged) in enumerate(spots):
        piece = refs[k]
        if staged:
            stage = held.pop(0)
            ins.append(pltpu.make_async_copy(piece, stage, sems.at[1, k]))
            piece = stage
        else:
            ins.append(None)
        to = pl.ds(pl.multiple_of(blocks[owner] * rows + at, 16), piece.shape[0])
        copies.append(pltpu.make_async_copy(piece, outs[out].at[to], sems.at[0, k]))
    for c in ins:
        if c is not None:
            c.start()
    for i, c in zip(ins, copies):
        if i is not None:
            i.wait()
        c.start()
    for c in copies:
        c.wait()


def place(rows, n, outs, pieces, staged):
    values = [p[0] for p in pieces]
    used = sorted({p[1] for p in pieces})
    spots = tuple((used.index(p[1]), p[2], p[3], staged) for p in pieces)
    cols = values[0].shape[1]
    given = [outs[k] for k in used if outs[k] is not None]
    done = pl.pallas_call(
        functools.partial(place_kernel, rows, len(used), spots),
        out_shape=tuple(pltpu.HBM((n * rows, cols), jnp.bfloat16) for _ in used),
        in_specs=[ANY if staged else VMEM] * len(values) + [ANY] * len(given),
        out_specs=(ANY,) * len(used),
        scratch_shapes=[
            *(pltpu.VMEM(v.shape, v.dtype) for v in values if staged),
            pltpu.SemaphoreType.DMA((2, len(values))),
        ],
        input_output_aliases={len(values) + k: k for k in range(len(given))},
        compiler_params=pltpu.CompilerParams(vmem_limit_bytes=8 << 20),
        name="place",
        cost_estimate=pl.CostEstimate(
            flops=0, bytes_accessed=sum(2 * v.size * 2 for v in values), transcendentals=0
        ),
    )(*map(in_hbm if staged else in_vmem, values), *map(in_hbm, given))
    outs = list(outs)
    for k, v in zip(used, done):
        outs[k] = v
    return outs


def body(train_gate, other_gate, train_up, other_up, router_weight, router_gain):
    n = lax.axis_size("fsdp")
    rows, _ = train_gate.shape[1:]

    def exchanged(name, value):
        flip = 3 if "w" in name else 1
        return lax.ppermute(value, "fsdp", [(i, i ^ flip) for i in range(n)])

    small, raw_near, raw_wide, gate, up = sums(
        train_gate[0],
        other_gate[0],
        train_up[0],
        other_up[0],
        router_weight.reshape(1, -1),
        router_gain.reshape(1, -1),
    )
    small_n = exchanged("sum_n", small)
    raw_n = exchanged("early_n", raw_near)
    pair = add_pair(small, small_n)
    pair_w = exchanged("sum_w", pair)
    raw_w = exchanged("early_w", raw_wide)

    at_gate = (0, RAW_WIDE, RAW_NEAR, rows - GATE_LAST)
    at_up = (0, rows - UP_LAST)
    gate0, scale_gate = ready_first(pair, pair_w, gate)
    gate0_n = exchanged("n0", gate0)
    gate0_w = exchanged("w0", gate0)
    up0, up1, gate1, gate_a, gate_b, scale_up = ready_rest(pair, pair_w, up, train_gate[0], other_gate[0])
    up0_n, up1_n, gate1_n = [exchanged(f"n{k}", v) for k, v in enumerate((up0, up1, gate1), 1)]
    gate_b_w, up0_w, up1_w, gate1_w = [exchanged(f"w{k}", v) for k, v in enumerate((gate_b, up0, up1, gate1), 1)]

    late, late_w, raw_n, raw_w, _ = lax.optimization_barrier((pair, pair_w, raw_n, raw_w, up1))
    copies = router_copies(late, late_w, lax.axis_size("ep"))
    columns = lax.all_to_all(copies, "ep", split_axis=0, concat_axis=0, tiled=True)
    serve_router = columns.reshape(columns.shape[0], -1).T

    gate_a_n, gate_b_n, gate_a_w = [
        (v / scale_gate).astype(jnp.bfloat16) for v in (raw_n[:RAW_WIDE], raw_n[RAW_WIDE:], raw_w)
    ]
    far_gate0 = exchanged("far_w0", gate0_n)
    far_up0 = exchanged("far_n0", up0_w)
    far_gate_b = exchanged("far_w1", gate_b_n)
    far_gate_a = exchanged("far_n1", gate_a_w)
    far_up1 = exchanged("far_n2", up1_w)
    far_gate1 = exchanged("far_w2", gate1_n)

    def gates(owner, *values):
        return [(v, 0, owner, at) for v, at in zip(values, at_gate) if v is not None]

    def ups(owner, *values):
        return [(v, 1, owner, at) for v, at in zip(values, at_up) if v is not None]

    groups = (
        gates("own", gate_a, gate_b, gate0, gate1) + ups("own", up0, up1),
        gates("near", gate_a_n, gate_b_n, gate0_n) + gates("wide", gate_a_w, gate_b_w, gate0_w),
        gates("near", None, None, None, gate1_n)
        + gates("wide", None, None, None, gate1_w)
        + ups("near", up0_n, up1_n)
        + ups("wide", up0_w, up1_w),
        gates("far", far_gate_a, far_gate_b, far_gate0) + ups("far", far_up0),
        gates("far", None, None, None, far_gate1) + ups("far", None, far_up1),
    )
    outs = [None, None]
    for k, group in enumerate(groups):
        outs = place(rows, n, outs, group, k < 3)
    return (outs[0][None], outs[1][None], scale_gate, scale_up, serve_router)


def solution(mesh):
    placed = (
        P("ep", "fsdp", None),
        P("ep", "fsdp", None),
        P("ep", "fsdp", None),
        P("ep", "fsdp", None),
        P("fsdp", "ep"),
        P("fsdp"),
    )
    return jax.shard_map(
        body,
        mesh=mesh,
        in_specs=placed,
        out_specs=(P("ep", None, None), P("ep", None, None), P("ep", None), P("ep", None), P()),
        check_vma=False,
    )
```
